32 devices in a mesh: fsdp: 8 (over y, x, core), tp: 4 (over z).
Axes of the slice: x: 2, y: 2, z: 4, core: 2. Of those that a mesh axis runs over, the one named last changes fastest.
Arguments:
- hidden_in: bfloat16 [4096, 8192], P('fsdp', 'tp'), may hold values from -480 to 480, as said below
- key_weight: bfloat16 [8192, 1024], P('tp', 'fsdp'), may hold values from -0.0625 to 0.0625
- norm_gain: float32 [8192], P('tp'), may hold values from 0.5 to 2
- key_grad: bfloat16 [4096, 1024], P(('fsdp', 'tp')), may hold values from -6 to 6
Outputs:
- key_states: bfloat16 [4096, 1024], P(('fsdp', 'tp'))
- input_grad: bfloat16 [4096, 8192], P('fsdp', 'tp')
- weight_grad: float32 [8192, 1024], P('tp', 'fsdp')
The draws below stay inside these ranges and needn't reach their ends.
Inputs may be any that keep to these rules, and one draw needn't show every extreme that they name: `hidden_in`: real values of either sign.
All inputs are finite; a program needn't handle non-finite values.
Results may differ from the reference program's by a relative error of at most 0.0049.
Values may be sent and summed in bfloat16 or wider, within the bound.
No kernel may reach another device: no remote copies, remote signals or barrier semaphores. Data moves between devices by JAX's collectives and lax.ppermute only.
A program may use at most 64 MiB of HBM per device.

```python
import math
import jax
import jax.numpy as jnp
from jax import lax

D = 8192
HEAD_DIM = 128
SEQ_LEN = 8192
TOK_G = 512
KD = 1024
TOKENS = 4096


def draw_hidden_in(key, part):
    subkeys = jax.random.split(key, 4)
    groups = TOKENS // TOK_G
    base_values = jnp.clip(jax.random.normal(subkeys[0], (TOKENS, D), jnp.float32), -4.0, 4.0)
    row_scale = jnp.exp(jax.random.uniform(subkeys[1], (TOKENS, 1), jnp.float32, 0.0, math.log(10.0)))
    column_scale = jnp.exp(jax.random.uniform(subkeys[2], (1, D), jnp.float32, math.log(0.3), math.log(3.0)))
    rising = jnp.exp(math.log(3.0) * jnp.arange(D, dtype=jnp.float32) / D)[None, :]
    partner = jax.random.permutation(subkeys[3], groups)
    row_group = jnp.arange(TOKENS, dtype=jnp.int32) // TOK_G
    column_group = jnp.arange(D, dtype=jnp.int32) // (D // groups)
    target = partner[row_group]
    factor = jnp.where(column_group[None, :] == target[:, None], 4.0, 1.0)
    values = jnp.clip(base_values * row_scale * column_scale * rising * factor, -480.0, 480.0)
    return values.astype(jnp.bfloat16)


def with_spikes(values, key, source, target, parts, factor):
    owner, partner = [(jnp.arange(values.shape[dim]) // (values.shape[dim] // parts)).reshape([-1 if axis == dim else 1 for axis in range(values.ndim)]) for dim in (source, target)]
    chosen = jax.random.permutation(key, parts)[partner]
    strong = (owner == chosen) | (owner == (partner + parts // 2) % parts)
    return jnp.where(strong, factor * values, values)


def block_levels(rng, extent, shards, smallest, largest):
    loudness = 1.0
    for dim, shards_of in shards:
        heights = jax.random.uniform(jax.random.fold_in(jax.random.fold_in(rng, 6), dim), (shards_of,), jnp.float32, smallest / len(shards), largest / len(shards))
        loudness = loudness * jnp.repeat(jnp.exp(heights), extent[dim] // shards_of).reshape((-1,) + (1,) * (len(extent) - 1 - dim))
    return loudness


def noise(key, shape, width, most, shards=(), kind=jnp.bfloat16):
    entries = jax.random.normal(key, shape, jnp.float32) * width
    if len(shards) > 0:
        entries = block_levels(key, shape, shards, -0.22, 0.18) * entries
    return jnp.clip(entries, min=-most, max=most).astype(kind)


def gaussian_with(own_key, shape, width, limit, cuts, heavy, kind=jnp.bfloat16):
    result = width * jax.random.normal(own_key, shape, jnp.float32)
    if cuts:
        result = result * block_levels(own_key, shape, cuts, -0.22, 0.18)
    return jnp.clip(with_spikes(result, jax.random.fold_in(own_key, 3), *heavy), -limit, limit).astype(kind)


def setup_inputs(seed: int = 0) -> dict:
    arg_keys = jax.random.split(jax.random.key(seed), 5)
    return {
        "hidden_in": draw_hidden_in(jax.random.fold_in(arg_keys[4], 71), 0),
        "key_weight": noise(arg_keys[1], (D, KD), D ** -0.5, 0.0625, ((0, 4), (1, 8))),
        "norm_gain": jnp.clip(jnp.exp(math.log(2.0) - 1.3862944 * jax.random.uniform(arg_keys[2], (D,), jnp.float32) ** block_levels(arg_keys[2], (D,), ((0, 4),), -0.2, 0.2)), 0.5, 2.0),
        "key_grad": gaussian_with(arg_keys[3], (TOKENS, KD), 1.0, 6.0, ((0, 32),), (0, 1, 32, 2.75)),
    }


ROPE_BASE = 500000.0
EPSILON = 1e-05

def angles_for(row_count, pair_count, row_start, pair_start):
    position = ((row_start + jnp.arange(row_count, dtype=jnp.int32)) % SEQ_LEN).astype(jnp.float32)
    within = (pair_start + jnp.arange(pair_count, dtype=jnp.int32)) % (HEAD_DIM // 2)
    frequency = jnp.power(jnp.float32(ROPE_BASE), -(2 * within).astype(jnp.float32) / HEAD_DIM)
    return position[:, None] * frequency[None, :]

def rotate(values, angles, direction):
    paired = values.reshape(values.shape[0], -1, 2)
    cosine = jnp.cos(angles)
    sine_part = direction * jnp.sin(angles)
    leading = paired[..., 0]
    second = paired[..., 1]
    turned = jnp.stack([leading * cosine - second * sine_part, leading * sine_part + second * cosine], -1)
    return turned.reshape(values.shape)

def reference(hidden_in, key_weight, norm_gain, key_grad):
    hidden_rows = hidden_in.astype(jnp.float32)
    inverse_rms = lax.rsqrt(lax.optimization_barrier(jnp.mean(hidden_rows * hidden_rows, -1, keepdims=True)) + EPSILON)
    normed = (hidden_rows * inverse_rms * norm_gain).astype(jnp.bfloat16)
    angles = angles_for(TOKENS, KD // 2, 0, 0)
    projected = jnp.dot(normed, key_weight, preferred_element_type=jnp.float32)
    key_states = rotate(projected, angles, 1.0).astype(jnp.bfloat16)
    grad_pre = rotate(key_grad.astype(jnp.float32), angles, -1.0).astype(jnp.bfloat16)
    grad_normed = lax.dot_general(grad_pre, key_weight, (((1,), (1,)), ((), ())), preferred_element_type=jnp.float32)
    scaled = grad_normed * norm_gain
    unit_rows = hidden_rows * inverse_rms
    input_grad = (inverse_rms * (scaled - unit_rows * lax.optimization_barrier(jnp.mean(scaled * unit_rows, -1, keepdims=True)))).astype(jnp.bfloat16)
    weight_grad = lax.dot_general(normed, grad_pre, (((0,), (0,)), ((), ())), preferred_element_type=jnp.float32)
    return (key_states, input_grad, weight_grad)
```

```python
import functools

import jax
import jax.numpy as jnp
from jax import lax
from jax.experimental import pallas as pl
from jax.experimental.pallas import tpu as pltpu
from jax.sharding import PartitionSpec as P

D = 8192
HEAD_DIM = 128
SEQ_LEN = 8192
ROPE_BASE = 500000.0
EPSILON = 1e-05
LANES = 128
STAT_ROWS = 8
VMEM = pltpu.VMEM
BF = jnp.bfloat16
F32 = jnp.float32


def angles_for(row_count, pair_count, row_start):
    position = ((row_start + jnp.arange(row_count, dtype=jnp.int32)) % SEQ_LEN).astype(F32)
    within = jnp.arange(pair_count, dtype=jnp.int32) % (HEAD_DIM // 2)
    frequency = jnp.power(F32(ROPE_BASE), -(2 * within).astype(F32) / HEAD_DIM)
    return position[:, None] * frequency[None, :]


def rotate(values, angles, direction):
    paired = values.reshape(values.shape[0], -1, 2)
    cosine = jnp.cos(angles)
    sine_part = direction * jnp.sin(angles)
    leading = paired[..., 0]
    second = paired[..., 1]
    turned = jnp.stack(
        [leading * cosine - second * sine_part, leading * sine_part + second * cosine], -1
    )
    return turned.reshape(values.shape)


def plain_body(hidden_in, key_weight, norm_gain, key_grad):
    hidden_rows = hidden_in.astype(F32)
    squares = lax.psum(jnp.sum(hidden_rows * hidden_rows, -1, keepdims=True), "tp")
    inverse_rms = lax.rsqrt(squares / D + EPSILON)
    normed = (hidden_rows * inverse_rms * norm_gain).astype(BF)
    weight_full = lax.all_gather(key_weight, "fsdp", axis=1, tiled=True)
    partial_value = jnp.dot(normed, weight_full, preferred_element_type=F32)
    projected = lax.psum_scatter(partial_value, "tp", scatter_dimension=0, tiled=True)
    group_rows = hidden_in.shape[0]
    local_rows = key_grad.shape[0]
    column_count = key_grad.shape[1]
    row_start = lax.axis_index("fsdp") * group_rows + lax.axis_index("tp") * local_rows
    angles = angles_for(local_rows, column_count // 2, row_start)
    key_states = rotate(projected, angles, 1.0).astype(BF)
    grad_pre = rotate(key_grad.astype(F32), angles, -1.0).astype(BF)
    grad_all = lax.all_gather(grad_pre, "tp", axis=0, tiled=True)
    grad_normed = lax.dot_general(
        grad_all, weight_full, (((1,), (1,)), ((), ())), preferred_element_type=F32
    )
    scaled = grad_normed * norm_gain
    unit_rows = hidden_rows * inverse_rms
    inner = lax.psum(jnp.sum(scaled * unit_rows, -1, keepdims=True), "tp")
    input_grad = (inverse_rms * (scaled - unit_rows * (inner / D))).astype(BF)
    term = lax.dot_general(
        normed, grad_all, (((0,), (0,)), ((), ())), preferred_element_type=F32
    )
    weight_grad = lax.psum_scatter(term, "fsdp", scatter_dimension=1, tiled=True)
    return (key_states, input_grad, weight_grad)


def turn(x, cosine, sine):
    lane = lax.broadcasted_iota(jnp.int32, x.shape, 1)
    ahead = pltpu.roll(x, x.shape[1] - 1, 1)
    behind = pltpu.roll(x, 1, 1)
    other = jnp.where(lane % 2 == 0, ahead, behind)
    return x * cosine + other * sine


def pack_stats(row, width):
    first = row.astype(BF).astype(F32)
    rest = row - first
    second = rest.astype(BF).astype(F32)
    third = rest - second
    if row.shape[1] < width:
        pad = jnp.zeros((1, width - row.shape[1]), F32)
        first, second, third = (jnp.concatenate([v, pad], 1) for v in (first, second, third))
    which = lax.broadcasted_iota(jnp.int32, (STAT_ROWS, width), 0)
    zero = jnp.zeros((STAT_ROWS, width), F32)
    block = jnp.where(which == 0, first, jnp.where(which == 1, second, jnp.where(which == 2, third, zero)))
    return block.astype(BF)


def sum_stats(refs, rows, count):
    total = jnp.zeros((1, count), F32)
    for ref in refs:
        block = ref[rows : rows + STAT_ROWS, :count].astype(F32)
        total = total + jnp.sum(block, 0, keepdims=True)
    return total


def as_column(row):
    return jnp.transpose(jnp.broadcast_to(row, (LANES, row.shape[1])))


def widen(column, width):
    return jnp.concatenate([column] * (width // LANES), 1)


def aligned(index, size):
    return pl.ds(pl.multiple_of(index * size, size), size)


def grad_kernel(grad_ref, cos_ref, sin_ref, stat_ref, out_ref):
    rows, width = grad_ref.shape
    cosine, sine = cos_ref[...], -sin_ref[...]
    for j in range(width // LANES):
        x = grad_ref[:, j * LANES : (j + 1) * LANES].astype(F32)
        out_ref[:rows, j * LANES : (j + 1) * LANES] = turn(x, cosine, sine).astype(BF)
    out_ref[rows:, :] = pack_stats(stat_ref[...], width)


def proj_kernel(tps, slots, ids, *refs):
    m_refs = refs[:tps]
    h_ref, gain_ref = refs[tps : tps + 2]
    w_refs = refs[tps + 2 : tps + 2 + 2 * slots]
    outs = refs[tps + 2 + 2 * slots :]
    q_refs = outs[:tps]
    w_full, normed, proj, inner_acc, sems = outs[tps:]
    f, t = ids[0], ids[1]
    rows = m_refs[0].shape[0] - STAT_ROWS
    tokens = rows * tps
    width = w_full.shape[1]
    block = w_refs[0].shape[1]
    copies = []
    for half in range(2):
        for j in range(slots):
            i = half * slots + j
            place = f ^ (2 * j + half)
            copies.append(
                pltpu.make_async_copy(w_refs[i], w_full.at[:, aligned(place, block)], sems.at[i])
            )
    for copy in copies:
        copy.start()
    total = sum_stats(m_refs, rows, tokens)
    inverse = as_column(lax.rsqrt(total / D + EPSILON))
    inner_acc[...] = inverse
    wide = h_ref.shape[1]

    def norm_step(i, _):
        at = aligned(i, rows)
        scale = widen(inner_acc[at, :], wide)
        normed[at, :] = (h_ref[at, :].astype(F32) * scale * gain_ref[...]).astype(BF)
        return 0

    lax.fori_loop(0, tps, norm_step, 0)
    inner_acc[...] = jnp.zeros_like(inner_acc)
    for copy in copies:
        copy.wait()
    tile = 2 * LANES

    def dot_step(n, _):
        at = aligned(n, tile)
        proj[:, at] = jnp.dot(normed[...], w_full[:, at], preferred_element_type=F32)
        for s in range(tps):
            rows_at = aligned(t ^ s, rows)
            product = proj[rows_at, at] * m_refs[s][:rows, at].astype(F32)
            inner_acc[rows_at, :] += product[:, :LANES] + product[:, LANES:]
        return 0

    lax.fori_loop(0, width // tile, dot_step, 0)
    inner = jnp.sum(jnp.transpose(inner_acc[...]), 0, keepdims=True)
    stats = pack_stats(inner, width)
    for s in range(tps):
        value = proj[aligned(t ^ s, rows), :]
        q_refs[s][:rows, :] = value.astype(q_refs[s].dtype)
        q_refs[s][rows:, :] = stats.astype(q_refs[s].dtype)


def wgrad_kernel(tps, slots, ids, *refs):
    m_refs = refs[:tps]
    p_refs = refs[tps : 2 * tps]
    h_ref, hp_ref, gain_ref = refs[2 * tps : 2 * tps + 3]
    own_ref, a_send, a_keep, b_send, b_keep, grad_t, scale = refs[2 * tps + 3 :]
    f, t = ids[0], ids[1]
    rows = m_refs[0].shape[0] - STAT_ROWS
    tokens = rows * tps
    block = LANES
    for which, group in enumerate((m_refs, p_refs)):
        total = sum_stats(group, rows, tokens)
        scale[which * tokens : (which + 1) * tokens, :] = as_column(lax.rsqrt(total / D + EPSILON))
        for s in range(tps):
            at = pl.ds(pl.multiple_of(which * tokens + (t ^ s) * rows, rows), rows)
            for j in range(slots):
                piece = group[s][:rows, aligned(f ^ (2 * j), block)]
                grad_t[j * block : (j + 1) * block, at] = jnp.transpose(piece)
    tile = 2 * LANES
    half_tiles = h_ref.shape[1] // tile // 2

    def product(n):
        at = aligned(n, tile)
        gain = gain_ref[:, at]
        factor = widen(scale[...], tile)
        upper = (h_ref[:, at].astype(F32) * factor[:tokens] * gain).astype(BF)
        lower = (hp_ref[:, at].astype(F32) * factor[tokens:] * gain).astype(BF)
        both = jnp.concatenate([upper, lower], 0)
        return jnp.dot(grad_t[...], both, preferred_element_type=F32)

    def first_half(n, _):
        value = product(n)
        at = aligned(n, tile)
        own_ref[:, at] = value[:block]
        a_send[:block, at] = value[block : 2 * block].astype(BF)
        a_send[block:, at] = value[3 * block :].astype(BF)
        a_keep[:, at] = value[2 * block : 3 * block]
        return 0

    def second_half(n, _):
        value = product(n + half_tiles)
        at = aligned(n, tile)
        own_ref[:, aligned(n + half_tiles, tile)] = value[:block]
        b_send[:, at] = value[2 * block :].astype(BF)
        b_keep[:, at] = value[block : 2 * block]
        return 0

    lax.fori_loop(0, half_tiles, first_half, 0)
    lax.fori_loop(0, half_tiles, second_half, 0)


def wsum_kernel(own_ref, a1_ref, a2_ref, b1_ref, b2_ref, out_ref):
    block, wide = own_ref.shape
    half = wide // 2
    for n in range(wide // LANES):
        at = slice(n * LANES, (n + 1) * LANES)
        if n * LANES < half:
            one, two, there = a1_ref, a2_ref, at
        else:
            one, two, there = b1_ref, b2_ref, slice(n * LANES - half, (n + 1) * LANES - half)
        value = own_ref[:, at] + one[:block, there].astype(F32) + two[:, there].astype(F32)
        out_ref[at, :] = jnp.transpose(value)


def keys_kernel(tps, *refs):
    q_refs = refs[:tps]
    cos_ref, sin_ref, out_ref = refs[tps:]
    rows, width = out_ref.shape
    cosine, sine = cos_ref[...], sin_ref[...]
    for j in range(width // LANES):
        at = slice(j * LANES, (j + 1) * LANES)
        x = q_refs[0][:rows, at].astype(F32)
        for ref in q_refs[1:]:
            x = x + ref[:rows, at].astype(F32)
        out_ref[:, at] = turn(x, cosine, sine).astype(BF)


def input_kernel(tps, slots, ids, *refs):
    m_refs = refs[:tps]
    q_refs = refs[tps : 2 * tps]
    h_ref, gain_ref = refs[2 * tps : 2 * tps + 2]
    w_refs = refs[2 * tps + 2 : 2 * tps + 2 + 2 * slots]
    out_ref, w_full, grad, scale, mean, sems = refs[2 * tps + 2 + 2 * slots :]
    f, t = ids[0], ids[1]
    rows = m_refs[0].shape[0] - STAT_ROWS
    tokens = rows * tps
    block = w_refs[0].shape[1]
    copies = []
    for half in range(2):
        for j in range(slots):
            i = half * slots + j
            place = f ^ (2 * j + half)
            copies.append(
                pltpu.make_async_copy(w_refs[i], w_full.at[:, aligned(place, block)], sems.at[i])
            )
    for copy in copies:
        copy.start()
    inverse = lax.rsqrt(sum_stats(m_refs, rows, tokens) / D + EPSILON)
    inner = sum_stats(q_refs, rows, tokens)
    scale[...] = as_column(inverse)
    mean[...] = as_column(inner / D)
    for s in range(tps):
        grad[aligned(t ^ s, rows), :] = m_refs[s][:rows, :]
    for copy in copies:
        copy.wait()
    tile = 2 * LANES

    def step(n, _):
        at = aligned(n, tile)
        value = lax.dot_general(
            grad[...], w_full[at, :], (((1,), (1,)), ((), ())), preferred_element_type=F32
        )
        inv = widen(scale[...], tile)
        unit = h_ref[:, at].astype(F32) * inv
        scaled = value * gain_ref[:, at]
        out_ref[:, at] = (inv * (scaled - unit * widen(mean[...], tile))).astype(BF)
        return 0

    lax.fori_loop(0, h_ref.shape[1] // tile, step, 0)


def shape(dims, dtype):
    return jax.ShapeDtypeStruct(dims, dtype)


def call(kernel, outs, operands, specs, scratch=(), flops=0, size=0, name=None):
    return pl.pallas_call(
        kernel,
        out_shape=outs,
        in_specs=specs,
        out_specs=jax.tree.map(lambda _: pl.BlockSpec(memory_space=VMEM), outs),
        scratch_shapes=list(scratch),
        compiler_params=pltpu.CompilerParams(vmem_limit_bytes=48 * 1024 * 1024),
        cost_estimate=pl.CostEstimate(flops=flops, bytes_accessed=size, transcendentals=0),
        name=name,
    )(*operands)


def staged_body(fsdp, tps, hidden, weight, gain, grad):
    slots = fsdp // 2
    tokens, wide = hidden.shape
    rows, width = grad.shape
    block = weight.shape[1]
    f = lax.axis_index("fsdp")
    t = lax.axis_index("tp")
    ids = jnp.stack([f, t]).astype(jnp.int32)

    def across(x, bit):
        return lax.ppermute(x, "fsdp", [(i, i ^ bit) for i in range(fsdp)])

    def along(x, bit):
        return lax.ppermute(x, "tp", [(i, i ^ bit) for i in range(tps)])

    vm = pl.BlockSpec(memory_space=VMEM)
    sm = pl.BlockSpec(memory_space=pltpu.SMEM)
    hb = pl.BlockSpec(memory_space=pltpu.HBM)

    half = wide // 2
    w_x = across(weight, 2)
    w_y = across(weight, 4)
    hidden_p = across(hidden, 1)

    squares = jnp.sum(jnp.square(hidden.astype(F32)), -1).reshape(1, tokens)
    lane = jnp.arange(HEAD_DIM, dtype=jnp.int32)
    frequency = jnp.power(F32(ROPE_BASE), -(2 * (lane // 2)).astype(F32) / HEAD_DIM)
    position = ((f * tokens + t * rows + jnp.arange(rows, dtype=jnp.int32)) % SEQ_LEN).astype(F32)
    angles = position[:, None] * frequency[None, :]
    cosine = jnp.cos(angles)
    sine = jnp.sin(angles) * jnp.where(lane % 2 == 0, F32(-1), F32(1))[None, :]
    message = call(
        grad_kernel, shape((rows + STAT_ROWS, width), BF), (grad, cosine, sine, squares), [vm] * 4,
        flops=10**6, size=10**6, name="grad",
    )
    own = [message] + [along(message, s) for s in range(1, tps)]
    partner = [across(m, 1) for m in own]

    w_d = jnp.concatenate([across(w_x[:half], 4), across(w_y[half:], 2)], 0)
    mine = [weight, w_x, w_y, w_d]
    weights = mine + [across(w, 1) for w in mine]

    gain_row = gain.reshape(1, wide)
    flops = 2 * tokens * wide * width
    q = call(
        functools.partial(proj_kernel, tps, slots),
        [shape((rows + STAT_ROWS, width), F32)] + [shape((rows + STAT_ROWS, width), BF)] * (tps - 1),
        (ids, *own, hidden, gain_row, *weights),
        [sm] + [vm] * (tps + 2) + [hb] * len(weights),
        [
            pltpu.VMEM((wide, width), BF),
            pltpu.VMEM((tokens, wide), BF),
            pltpu.VMEM((tokens, width), F32),
            pltpu.VMEM((tokens, LANES), F32),
            pltpu.SemaphoreType.DMA((len(weights),)),
        ],
        flops=flops, size=8 * 10**6, name="proj",
    )
    q = [q[0]] + [along(q[s], s) for s in range(1, tps)]

    own_w, a_send, a_keep, b_send, b_keep = call(
        functools.partial(wgrad_kernel, tps, slots),
        [
            shape((block, wide), F32),
            shape((2 * block, half), BF),
            shape((block, half), F32),
            shape((2 * block, half), BF),
            shape((block, half), F32),
        ],
        (ids, *own, *partner, hidden, hidden_p, gain_row),
        [sm] + [vm] * (2 * tps + 3),
        [pltpu.VMEM((slots * block, 2 * tokens), BF), pltpu.VMEM((2 * tokens, LANES), F32)],
        flops=flops, size=8 * 10**6, name="wgrad",
    )
    a_one = across(a_send, 2)
    b_one = across(b_send, 4)
    a_two = across((a_keep + a_one[block:].astype(F32)).astype(BF), 4)
    b_two = across((b_keep + b_one[block:].astype(F32)).astype(BF), 2)

    key_states = call(
        functools.partial(keys_kernel, tps), shape((rows, width), BF), (*q, cosine, sine),
        [vm] * (tps + 2), flops=10**6, size=10**6, name="keys",
    )
    input_grad = call(
        functools.partial(input_kernel, tps, slots),
        shape((tokens, wide), BF),
        (ids, *own, *q, hidden, gain_row, *weights),
        [sm] + [vm] * (2 * tps + 2) + [hb] * len(weights),
        [
            pltpu.VMEM((wide, width), BF),
            pltpu.VMEM((tokens, width), BF),
            pltpu.VMEM((tokens, LANES), F32),
            pltpu.VMEM((tokens, LANES), F32),
            pltpu.SemaphoreType.DMA((len(weights),)),
        ],
        flops=flops, size=8 * 10**6, name="input",
    )
    weight_grad = call(
        wsum_kernel, shape((wide, block), F32), (own_w, a_one, a_two, b_one, b_two), [vm] * 5,
        flops=10**6, size=3 * 10**6, name="wsum",
    )
    return key_states, input_grad, weight_grad


def fits(fsdp, tps, hidden, weight, gain, grad):
    return (
        fsdp == 2 * 4
        and tps & (tps - 1) == 0
        and weight.shape[1] == LANES == HEAD_DIM
        and grad.shape[0] % LANES == 0
        and hidden.shape[1] % (4 * LANES) == 0
        and hidden.shape[0] <= grad.shape[1]
    )


def solution(mesh):
    fsdp, tps = mesh.shape["fsdp"], mesh.shape["tp"]

    def body(*arrays):
        if fits(fsdp, tps, *arrays):
            return staged_body(fsdp, tps, *arrays)
        return plain_body(*arrays)

    in_specs = (P("fsdp", "tp"), P("tp", "fsdp"), P("tp"), P(("fsdp", "tp"), None))
    out_specs = (P(("fsdp", "tp"), None), P("fsdp", "tp"), P("tp", "fsdp"))
    return jax.shard_map(body, mesh=mesh, in_specs=in_specs, out_specs=out_specs, check_vma=False)
```
